32 devices in a mesh: section: 2 (over core), dp: 8 (over z, x), tensor: 2 (over y).
Axes of the slice: x: 2, y: 2, z: 4, core: 2. Of those that a mesh axis runs over, the one named last changes fastest.
Arguments:
- tokens: bfloat16 [1024, 4096], P('dp', 'tensor'), may hold values from -6 to 6
- gain: bfloat16 [2, 4096], P('section', 'tensor'), may hold values from 0.099609375 to 1.8984375
- w_up: bfloat16 [2, 4096, 5120], P('section', 'dp', 'tensor'), may hold values from -0.09375 to 0.09375
- w_down: bfloat16 [2, 5120, 4096], P('section', 'tensor', 'dp'), may hold values from -0.078125 to 0.078125
- cotangent: bfloat16 [2, 1024, 4096], P('section', 'dp'), may hold values from -6 to 6
Outputs:
- states: bfloat16 [2, 1024, 4096], P('section', 'dp', 'tensor')
- grad_down: bfloat16 [2, 5120, 4096], P('section', 'tensor', 'dp')
The draws below stay inside these ranges and needn't reach their ends.
All inputs are finite; a program needn't handle non-finite values.
Results may differ from the reference program's by a relative error of at most 0.02.
Values may be sent and summed in bfloat16 or wider, within the bound.
A program may use at most 128 MiB of HBM per device.

```python
import jax
import jax.numpy as jnp
from jax import lax

WIDTH = 4096
HIDDEN_SIZE = 5120
TOK_DEV = 128
TOKENS = 1024
LAYERS = 2
N_SECTION = 2
N_DP = 8
N_TENSOR = 2


def block_levels(own_key, dims, pieces, low, high):
    level = 1.0
    for dim, blocks in pieces:
        steps = jax.random.uniform(jax.random.fold_in(jax.random.fold_in(own_key, 6), dim), (blocks,), jnp.float32, low / len(pieces), high / len(pieces))
        level = level * jnp.repeat(jnp.exp(steps), dims[dim] // blocks).reshape((-1,) + (1,) * (len(dims) - 1 - dim))
    return level


def normal_values(key, extent, deviation, bound, cuts=(), dtype=jnp.bfloat16):
    drawn = deviation * jax.random.normal(key, extent, jnp.float32)
    if cuts:
        drawn = drawn * block_levels(key, extent, cuts, -0.22, 0.18)
    return jnp.clip(drawn, -bound, bound).astype(dtype)


def setup_inputs(seed: int = 0) -> dict:
    arg_keys = jax.random.split(jax.random.key(seed), 6)
    return {
        "tokens": normal_values(arg_keys[0], (TOKENS, WIDTH), 1.0, 6.0, ((0, 8), (1, 2))),
        "gain": jnp.clip(1.0 + 0.18 * jax.random.normal(arg_keys[1], (LAYERS, WIDTH), jnp.float32), 0.099609375, 1.8984375).astype(jnp.bfloat16),
        "w_up": normal_values(arg_keys[2], (LAYERS, WIDTH, HIDDEN_SIZE), WIDTH ** -0.5, 0.09375, ((0, 2), (1, 8), (2, 2))),
        "w_down": normal_values(arg_keys[3], (LAYERS, HIDDEN_SIZE, WIDTH), HIDDEN_SIZE ** -0.5, 0.078125, ((0, 2), (1, 2), (2, 8))),
        "cotangent": normal_values(arg_keys[4], (LAYERS, TOKENS, WIDTH), 1.0, 6.0, ((0, 2), (1, 8))),
    }


EPS = 1e-06

def layer_ref(acts, gain_row, up_mat, down_mat):
    acts_f = acts.astype(jnp.float32)
    mean_sq = lax.optimization_barrier(jnp.mean(acts_f * acts_f, axis=1, keepdims=True))
    normed = (acts_f * lax.rsqrt(mean_sq + EPS) * gain_row.astype(jnp.float32)).astype(jnp.bfloat16)
    pre_act = jnp.dot(normed, up_mat, preferred_element_type=jnp.float32)
    hidden = jax.nn.gelu(pre_act, approximate=True).astype(jnp.bfloat16)
    group_width = HIDDEN_SIZE // N_TENSOR
    summed = jnp.zeros(acts.shape, jnp.float32)
    for group_id in range(N_TENSOR):
        lower = group_id * group_width
        partial_value = jnp.dot(hidden[:, lower:lower + group_width], down_mat[lower:lower + group_width, :], preferred_element_type=jnp.float32).astype(jnp.bfloat16)
        summed = summed + lax.optimization_barrier(partial_value).astype(jnp.float32)
    return ((acts_f + summed).astype(jnp.bfloat16), hidden)

def reference(tokens, gain, w_up, w_down, cotangent):
    acts = tokens
    states = []
    grads = []
    for layer_id in range(N_SECTION):
        acts, hidden = layer_ref(acts, gain[layer_id], w_up[layer_id], w_down[layer_id])
        states.append(acts)
        grad_sum = jnp.zeros((HIDDEN_SIZE, WIDTH), jnp.float32)
        for peer_id in range(N_DP):
            lower = peer_id * TOK_DEV
            partial_value = lax.dot_general(hidden[lower:lower + TOK_DEV], cotangent[layer_id][lower:lower + TOK_DEV], (((0,), (0,)), ((), ())), preferred_element_type=jnp.float32).astype(jnp.bfloat16)
            grad_sum = grad_sum + lax.optimization_barrier(partial_value).astype(jnp.float32)
        grads.append(grad_sum.astype(jnp.bfloat16))
    return (jnp.stack(states), jnp.stack(grads))
```

```python
import jax
import jax.numpy as jnp
from jax import lax
from jax.sharding import PartitionSpec as P

EPS = 1e-06
F32 = jnp.float32
BF16 = jnp.bfloat16


def body(tokens, gain, w_up, w_down, cotangent):
    core = lax.axis_index("section")
    layers = lax.axis_size("section")
    assert layers == 2
    dp_id = lax.axis_index("dp")
    dp_count = lax.axis_size("dp")
    tensor_id = lax.axis_index("tensor")
    tensor_count = lax.axis_size("tensor")
    rows, own_width = tokens.shape
    width = own_width * tensor_count
    slice_width = width // dp_count
    hidden_width = w_up.shape[2]
    half = hidden_width // layers
    other = 1 - core
    all_rows = rows * dp_count

    def swap(array):
        return lax.ppermute(array, "section", [(0, 1), (1, 0)])

    def both(own, got):
        return (jnp.where(core == 0, own, got), jnp.where(core == 0, got, own))

    cot_mine = lax.all_to_all(cotangent[0], "dp", split_axis=1, concat_axis=0, tiled=True)

    half_rows = rows // layers
    tok_half = lax.dynamic_slice_in_dim(tokens, core * half_rows, half_rows, 0)
    tok_full = lax.all_gather(tok_half, "tensor", axis=1, tiled=True)
    tok_f = tok_full.astype(F32)
    sums_half = jnp.sum(tok_f * tok_f, axis=1)
    sums_a, sums_b = both(sums_half, swap(sums_half))
    sums = jnp.concatenate([sums_a, sums_b])
    x_half = lax.all_to_all(tok_full, "dp", split_axis=1, concat_axis=0, tiled=True)
    x_a, x_b = both(x_half, swap(x_half))
    x = jnp.concatenate(
        [
            x_a.reshape(dp_count, half_rows, slice_width),
            x_b.reshape(dp_count, half_rows, slice_width),
        ],
        axis=1,
    ).reshape(all_rows, slice_width)

    gain_all = lax.all_gather(gain, "tensor", axis=1, tiled=True)
    gain_own = lax.dynamic_slice_in_dim(gain_all, dp_id * slice_width, slice_width, 1)
    gains = both(gain_own, swap(gain_own))

    up_parts = both(
        lax.dynamic_slice_in_dim(w_up[0], core * half, half, 1),
        swap(lax.dynamic_slice_in_dim(w_up[0], other * half, half, 1)),
    )
    down_parts = both(
        lax.dynamic_slice_in_dim(w_down[0], core * half, half, 0),
        swap(lax.dynamic_slice_in_dim(w_down[0], other * half, half, 0)),
    )

    states = []
    hiddens = []
    for layer in range(layers):
        x_f = x.astype(F32)
        if layer > 0:
            sums = lax.psum_scatter(
                jnp.sum(x_f * x_f, axis=1), "dp", scatter_dimension=0, tiled=True
            )
        scaled = (x_f * gains[layer].astype(F32)).astype(BF16)
        part = jnp.dot(scaled, up_parts[layer], preferred_element_type=F32).astype(BF16)
        pre = lax.psum_scatter(part, "dp", scatter_dimension=0, tiled=True)
        inverse_rms = lax.rsqrt(sums / width + EPS)
        hidden = jax.nn.gelu(pre.astype(F32) * inverse_rms[:, None], approximate=True).astype(BF16)
        hidden_all = lax.all_gather(hidden, "dp", axis=0, tiled=True)
        hiddens.append(hidden_all)
        out = jnp.dot(hidden_all, down_parts[layer], preferred_element_type=F32)
        mid = all_rows // layers
        keep = lax.dynamic_slice_in_dim(out, core * mid, mid, 0)
        give = lax.dynamic_slice_in_dim(out, other * mid, mid, 0).astype(BF16)
        summed = keep + swap(give).astype(F32)
        if tensor_count == 2:
            sent = summed.astype(BF16)
            got = lax.ppermute(sent, "tensor", [(0, 1), (1, 0)])
            summed = sent.astype(F32) + got.astype(F32)
        else:
            summed = lax.psum(summed.astype(BF16), "tensor").astype(F32)
        x_mid = lax.dynamic_slice_in_dim(x_f, core * mid, mid, 0)
        new_mid = (x_mid + summed).astype(BF16)
        new_a, new_b = both(new_mid, swap(new_mid))
        x = jnp.concatenate([new_a, new_b], axis=0)
        states.append(x)

    state_own = jnp.where(core == 0, states[0], states[1])
    state_rows = lax.all_to_all(state_own, "dp", split_axis=0, concat_axis=1, tiled=True)
    state = lax.dynamic_slice_in_dim(state_rows, tensor_id * own_width, own_width, 1)

    hid_keep = jnp.where(core == 0, hiddens[0], hiddens[1])
    hid_got = swap(jnp.where(core == 0, hiddens[1], hiddens[0]))
    hid_parts = both(hid_keep, hid_got)
    hidden_whole = jnp.concatenate(hid_parts, axis=1)
    grad = lax.dot_general(
        hidden_whole, cot_mine, (((0,), (0,)), ((), ())), preferred_element_type=F32
    ).astype(BF16)
    return (state[None], grad[None])


def solution(mesh):
    placed = (
        P("dp", "tensor"),
        P("section", "tensor"),
        P("section", "dp", "tensor"),
        P("section", "tensor", "dp"),
        P("section", "dp", None),
    )
    return jax.shard_map(
        body,
        mesh=mesh,
        in_specs=placed,
        out_specs=(P("section", "dp", "tensor"), P("section", "tensor", "dp")),
        check_vma=False,
    )
```

```python
import functools

import jax
import jax.numpy as jnp
from jax import lax
from jax.experimental import pallas as pl
from jax.experimental.pallas import tpu as pltpu
from jax.sharding import PartitionSpec as P

EPS = 1e-06
F32 = jnp.float32
BF16 = jnp.bfloat16


MESH = pl.DeviceIdType.MESH
ROW_CHUNK = 16


def far_first(count):
    return sorted(range(1, count), key=lambda k: abs(2 * k - count)) + [0]


def remote(src, dst, send_sem, recv_sem, target):
    return pltpu.make_async_remote_copy(
        src_ref=src,
        dst_ref=dst,
        send_sem=send_sem,
        recv_sem=recv_sem,
        device_id=target,
        device_id_type=MESH,
    )


def layer_kernel(
    dp_count,
    inner,
    width,
    x_ref,
    gain_ref,
    up_ref,
    hid_out,
    scaled,
    sum_send,
    sum_recv,
    x_send,
    x_recv,
    z_send,
    z_recv,
    total,
    hid,
    sum_ss,
    sum_rs,
    x_ss,
    x_rs,
    z_ss,
    z_rs,
    up_ss,
    up_rs,
    dn_ss,
    dn_rs,
    fx_ss,
    fx_rs,
    out_sem,
):
    outer = dp_count // inner
    me = lax.axis_index("dp")
    z = me // inner
    x = lax.rem(me, inner)
    peer = 1 - x
    rows = x_ref.shape[1]

    barrier = pltpu.get_barrier_semaphore()
    for m in range(1, dp_count):
        pl.semaphore_signal(
            barrier, inc=1, device_id={"dp": lax.rem(me + m, dp_count)}, device_id_type=MESH
        )
    pl.semaphore_wait(barrier, dp_count - 1)

    row_id = lax.broadcasted_iota(jnp.int32, (rows, rows), 0)
    col_id = lax.broadcasted_iota(jnp.int32, (rows, rows), 1)
    eye = row_id == col_id
    gain_f = gain_ref[...].astype(F32)

    def prepare(block, _):
        values = x_ref[block].astype(F32)
        scaled[block] = (values * gain_f).astype(BF16)
        column = jnp.sum(values * values, axis=1, keepdims=True)
        sum_send[block] = jnp.sum(jnp.where(eye, column, 0.0), axis=0, keepdims=True)
        return 0

    lax.fori_loop(0, dp_count, prepare, 0)

    order = far_first(outer)
    x_copies = {}
    for k in order:
        zz = lax.rem(z + k, outer)
        x_send[k] = jnp.dot(
            scaled[zz * inner + peer], up_ref[...], preferred_element_type=F32
        ).astype(BF16)
        x_copies[k] = remote(
            x_send.at[k], x_recv.at[k], x_ss.at[k], x_rs.at[k], {"dp": z * inner + peer}
        )
        x_copies[k].start()
    sum_copies = []
    for m in range(1, dp_count):
        target = lax.rem(me + m, dp_count)
        copy = remote(
            sum_send.at[target], sum_recv.at[m], sum_ss.at[m], sum_rs.at[m], {"dp": target}
        )
        copy.start()
        sum_copies.append(copy)
    z_copies = {}
    for k in order:
        zz = lax.rem(z + k, outer)
        mine = jnp.dot(scaled[zz * inner + x], up_ref[...], preferred_element_type=F32)
        x_copies[k].wait_recv()
        if k == 0:
            total[...] = mine + x_recv[k].astype(F32)
        else:
            z_send[k] = (mine + x_recv[k].astype(F32)).astype(BF16)
            z_copies[k] = remote(
                z_send.at[k], z_recv.at[k], z_ss.at[k], z_rs.at[k], {"dp": zz * inner + x}
            )
            z_copies[k].start()
    sums = sum_send[me]
    for m in range(1, dp_count):
        sum_copies[m - 1].wait_recv()
        sums = sums + sum_recv[m]
    inverse = lax.rsqrt(jnp.sum(jnp.where(eye, sums, 0.0), axis=1, keepdims=True) / width + EPS)
    for k in order[:-1]:
        z_copies[k].wait_recv()

    for lower in range(0, rows, ROW_CHUNK):
        rows_now = pl.ds(lower, ROW_CHUNK)
        value = total[rows_now]
        for k in order[:-1]:
            value = value + z_recv[k, rows_now].astype(F32)
        value = value * inverse[lower : lower + ROW_CHUNK]
        hid[me, rows_now] = jax.nn.gelu(value, approximate=True).astype(BF16)

    def forward(origin, sem_id):
        return remote(
            hid.at[origin * inner + x],
            hid.at[origin * inner + x],
            fx_ss.at[sem_id],
            fx_rs.at[sem_id],
            {"dp": z * inner + peer},
        )

    def expect(origin, sem_id):
        return remote(
            hid.at[origin * inner + peer],
            hid.at[origin * inner + peer],
            fx_ss.at[sem_id],
            fx_rs.at[sem_id],
            {"dp": z * inner + peer},
        )

    def hop(origin, target, sends, recvs, j):
        return remote(
            hid.at[origin * inner + x],
            hid.at[origin * inner + x],
            sends.at[j],
            recvs.at[j],
            {"dp": target * inner + x},
        )

    def landing(origin, sends, recvs, j):
        return remote(
            hid.at[origin * inner + x],
            hid.at[origin * inner + x],
            sends.at[j],
            recvs.at[j],
            {"dp": z * inner + peer},
        )

    def store(block):
        return pltpu.make_async_copy(hid.at[block], hid_out.at[block], out_sem.at[block])

    last = outer - 1
    for j in range(outer):
        if j < last:

            @pl.when((z - j >= 0) & (z < last))
            def _():
                hop(z - j, z + 1, up_ss, up_rs, j).start()

            @pl.when((z + j <= last) & (z > 0))
            def _():
                hop(z + j, z - 1, dn_ss, dn_rs, j).start()

        if j == 0:
            forward(z, 0).start()
            store(me).start()
        if j < last:

            @pl.when(z - 1 - j >= 0)
            def _():
                landing(z - 1 - j, up_ss, up_rs, j).wait_recv()
                forward(z - 1 - j, 1 + j).start()
                store((z - 1 - j) * inner + x).start()

            @pl.when(z + 1 + j <= last)
            def _():
                landing(z + 1 + j, dn_ss, dn_rs, j).wait_recv()
                forward(z + 1 + j, outer + j).start()
                store((z + 1 + j) * inner + x).start()

    expect(z, 0).wait_recv()
    store(z * inner + peer).start()
    for j in range(last):

        @pl.when(z - 1 - j >= 0)
        def _():
            expect(z - 1 - j, 1 + j).wait_recv()
            store((z - 1 - j) * inner + peer).start()

        @pl.when(z + 1 + j <= last)
        def _():
            expect(z + 1 + j, outer + j).wait_recv()
            store((z + 1 + j) * inner + peer).start()

    for copy in list(x_copies.values()) + list(z_copies.values()) + sum_copies:
        copy.wait_send()
    forward(z, 0).wait_send()
    for j in range(last):

        @pl.when((z - j >= 0) & (z < last))
        def _():
            hop(z - j, z + 1, up_ss, up_rs, j).wait_send()

        @pl.when((z + j <= last) & (z > 0))
        def _():
            hop(z + j, z - 1, dn_ss, dn_rs, j).wait_send()

        @pl.when(z - 1 - j >= 0)
        def _():
            forward(z - 1 - j, 1 + j).wait_send()

        @pl.when(z + 1 + j <= last)
        def _():
            forward(z + 1 + j, outer + j).wait_send()

    for block in range(dp_count):
        store(block).wait()


def layer_hidden(layer, dp_count, width, x, gain_row, up):
    rows = x.shape[0] // dp_count
    slice_width = x.shape[1]
    half = up.shape[1]
    inner = 2
    assert dp_count % inner == 0
    outer = dp_count // inner
    dma = pltpu.SemaphoreType.DMA
    vmem = pl.BlockSpec(memory_space=pltpu.VMEM)
    wide = pltpu.VMEM((outer, rows, half), BF16)
    hidden = pl.pallas_call(
        functools.partial(layer_kernel, dp_count, inner, width),
        name=f"layer{layer}",
        out_shape=jax.ShapeDtypeStruct((dp_count, rows, half), BF16),
        in_specs=[vmem] * 3,
        out_specs=pl.BlockSpec(memory_space=pl.ANY),
        scratch_shapes=[
            pltpu.VMEM((dp_count, rows, slice_width), BF16),
            pltpu.VMEM((dp_count, 1, rows), F32),
            pltpu.VMEM((dp_count, 1, rows), F32),
            wide,
            wide,
            wide,
            wide,
            pltpu.VMEM((rows, half), F32),
            pltpu.VMEM((dp_count, rows, half), BF16),
        ]
        + [dma((dp_count,))] * 2
        + [dma((outer,))] * 8
        + [dma((2 * outer,))] * 2
        + [dma((dp_count,))],
        compiler_params=pltpu.CompilerParams(collective_id=layer, has_side_effects=True),
    )(x.reshape(dp_count, rows, slice_width), gain_row, up)
    return hidden.reshape(dp_count * rows, half)


def body(tokens, gain, w_up, w_down, cotangent):
    core = lax.axis_index("section")
    layers = lax.axis_size("section")
    assert layers == 2
    dp_id = lax.axis_index("dp")
    dp_count = lax.axis_size("dp")
    tensor_id = lax.axis_index("tensor")
    tensor_count = lax.axis_size("tensor")
    rows, own_width = tokens.shape
    width = own_width * tensor_count
    slice_width = width // dp_count
    hidden_width = w_up.shape[2]
    half = hidden_width // layers
    other = 1 - core
    all_rows = rows * dp_count

    def swap(array):
        return lax.ppermute(array, "section", [(0, 1), (1, 0)])

    def both(own, got):
        return (jnp.where(core == 0, own, got), jnp.where(core == 0, got, own))

    cot_mine = lax.all_to_all(cotangent[0], "dp", split_axis=1, concat_axis=0, tiled=True)

    half_rows = rows // layers
    tok_half = lax.dynamic_slice_in_dim(tokens, core * half_rows, half_rows, 0)
    tok_full = lax.all_gather(tok_half, "tensor", axis=1, tiled=True)
    x_half = lax.all_to_all(tok_full, "dp", split_axis=1, concat_axis=0, tiled=True)
    x_a, x_b = both(x_half, swap(x_half))
    x = jnp.concatenate(
        [
            x_a.reshape(dp_count, half_rows, slice_width),
            x_b.reshape(dp_count, half_rows, slice_width),
        ],
        axis=1,
    ).reshape(all_rows, slice_width)

    gain_all = lax.all_gather(gain, "tensor", axis=1, tiled=True)
    gain_own = lax.dynamic_slice_in_dim(gain_all, dp_id * slice_width, slice_width, 1)
    gains = both(gain_own, swap(gain_own))

    up_parts = both(
        lax.dynamic_slice_in_dim(w_up[0], core * half, half, 1),
        swap(lax.dynamic_slice_in_dim(w_up[0], other * half, half, 1)),
    )
    down_parts = both(
        lax.dynamic_slice_in_dim(w_down[0], core * half, half, 0),
        swap(lax.dynamic_slice_in_dim(w_down[0], other * half, half, 0)),
    )

    states = []
    hiddens = []
    for layer in range(layers):
        x_f = x.astype(F32)
        hidden_all = layer_hidden(layer, dp_count, width, x, gains[layer], up_parts[layer])
        hiddens.append(hidden_all)
        out = jnp.dot(hidden_all, down_parts[layer], preferred_element_type=F32)
        mid = all_rows // layers
        keep = lax.dynamic_slice_in_dim(out, core * mid, mid, 0)
        give = lax.dynamic_slice_in_dim(out, other * mid, mid, 0).astype(BF16)
        summed = keep + swap(give).astype(F32)
        if tensor_count == 2:
            sent = summed.astype(BF16)
            got = lax.ppermute(sent, "tensor", [(0, 1), (1, 0)])
            summed = sent.astype(F32) + got.astype(F32)
        else:
            summed = lax.psum(summed.astype(BF16), "tensor").astype(F32)
        x_mid = lax.dynamic_slice_in_dim(x_f, core * mid, mid, 0)
        new_mid = (x_mid + summed).astype(BF16)
        new_a, new_b = both(new_mid, swap(new_mid))
        x = jnp.concatenate([new_a, new_b], axis=0)
        states.append(x)

    state_own = jnp.where(core == 0, states[0], states[1])
    state_rows = lax.all_to_all(state_own, "dp", split_axis=0, concat_axis=1, tiled=True)
    state = lax.dynamic_slice_in_dim(state_rows, tensor_id * own_width, own_width, 1)

    hid_keep = jnp.where(core == 0, hiddens[0], hiddens[1])
    hid_got = swap(jnp.where(core == 0, hiddens[1], hiddens[0]))
    hid_parts = both(hid_keep, hid_got)
    hidden_whole = jnp.concatenate(hid_parts, axis=1)
    grad = lax.dot_general(
        hidden_whole, cot_mine, (((0,), (0,)), ((), ())), preferred_element_type=F32
    ).astype(BF16)
    return (state[None], grad[None])


def solution(mesh):
    placed = (
        P("dp", "tensor"),
        P("section", "tensor"),
        P("section", "dp", "tensor"),
        P("section", "tensor", "dp"),
        P("section", "dp", None),
    )
    return jax.shard_map(
        body,
        mesh=mesh,
        in_specs=placed,
        out_specs=(P("section", "dp", "tensor"), P("section", "tensor", "dp")),
        check_vma=False,
    )
```

```python
import functools

import jax
import jax.numpy as jnp
from jax import lax
from jax.experimental import pallas as pl
from jax.experimental.pallas import tpu as pltpu
from jax.sharding import PartitionSpec as P

EPS = 1e-06
F32 = jnp.float32
BF16 = jnp.bfloat16


MESH = pl.DeviceIdType.MESH
ROW_CHUNK = 16


def far_first(count):
    return sorted(range(1, count), key=lambda k: abs(2 * k - count)) + [0]


def remote(src, dst, send_sem, recv_sem, target):
    return pltpu.make_async_remote_copy(
        src_ref=src,
        dst_ref=dst,
        send_sem=send_sem,
        recv_sem=recv_sem,
        device_id=target,
        device_id_type=MESH,
    )


def layer_kernel(
    sizes,
    inner,
    width,
    layer,
    is_last,
    x_ref,
    gain_ref,
    up_ref,
    down_ref,
    hid_out,
    x_out,
    state_out,
    scaled,
    sum_send,
    sum_recv,
    x_send,
    x_recv,
    z_send,
    z_recv,
    total,
    hid,
    part_send,
    part_recv,
    x_next,
    state_buf,
    sum_ss,
    sum_rs,
    x_ss,
    x_rs,
    z_ss,
    z_rs,
    up_ss,
    up_rs,
    dn_ss,
    dn_rs,
    fx_ss,
    fx_rs,
    out_sem,
    part_ss,
    part_rs,
    xn_ss,
    xn_rs,
    st_ss,
    st_rs,
    end_sem,
):
    sections, dp_count, tensors = sizes
    outer = dp_count // inner
    group = sections * tensors
    owned = dp_count // group
    per_tensor = dp_count // tensors
    core = lax.axis_index("section")
    tensor = lax.axis_index("tensor")
    member = tensor * sections + core
    me = lax.axis_index("dp")
    z = me // inner
    x = lax.rem(me, inner)
    peer = 1 - x
    rows = x_ref.shape[1]

    barrier = pltpu.get_barrier_semaphore()
    for m in range(1, dp_count):
        pl.semaphore_signal(
            barrier, inc=1, device_id={"dp": lax.rem(me + m, dp_count)}, device_id_type=MESH
        )

    def place(index):
        return {"section": lax.rem(index, sections), "tensor": index // sections}

    for off in range(1, group):
        pl.semaphore_signal(
            barrier, inc=1, device_id=place(lax.rem(member + off, group)), device_id_type=MESH
        )
    giver = lax.rem(me, group)
    for q in range(per_tensor):
        source = tensor * per_tensor + q
        apart = (giver != member) | (source != me)

        @pl.when((core == layer) & apart)
        def _():
            pl.semaphore_signal(
                barrier, inc=1, device_id={"dp": source, **place(giver)}, device_id_type=MESH
            )

    def state_is_local(block):
        return (core == layer) & (block == me) & (tensor == me // per_tensor)

    arrivals = dp_count - 1 + group - 1 + owned
    for i in range(owned):
        arrivals = arrivals - state_is_local(member + i * group).astype(jnp.int32)
    pl.semaphore_wait(barrier, arrivals)

    row_id = lax.broadcasted_iota(jnp.int32, (rows, rows), 0)
    col_id = lax.broadcasted_iota(jnp.int32, (rows, rows), 1)
    eye = row_id == col_id
    gain_f = gain_ref[...].astype(F32)

    def prepare(block, _):
        values = x_ref[block].astype(F32)
        scaled[block] = (values * gain_f).astype(BF16)
        column = jnp.sum(values * values, axis=1, keepdims=True)
        sum_send[block] = jnp.sum(jnp.where(eye, column, 0.0), axis=0, keepdims=True)
        return 0

    lax.fori_loop(0, dp_count, prepare, 0)

    order = far_first(outer)
    x_copies = {}
    for k in order:
        zz = lax.rem(z + k, outer)
        x_send[k] = jnp.dot(
            scaled[zz * inner + peer], up_ref[...], preferred_element_type=F32
        ).astype(BF16)
        x_copies[k] = remote(
            x_send.at[k], x_recv.at[k], x_ss.at[k], x_rs.at[k], {"dp": z * inner + peer}
        )
        x_copies[k].start()
    sum_copies = []
    for m in range(1, dp_count):
        target = lax.rem(me + m, dp_count)
        copy = remote(
            sum_send.at[target], sum_recv.at[m], sum_ss.at[m], sum_rs.at[m], {"dp": target}
        )
        copy.start()
        sum_copies.append(copy)
    z_copies = {}
    for k in order:
        zz = lax.rem(z + k, outer)
        mine = jnp.dot(scaled[zz * inner + x], up_ref[...], preferred_element_type=F32)
        x_copies[k].wait_recv()
        if k == 0:
            total[...] = mine + x_recv[k].astype(F32)
        else:
            z_send[k] = (mine + x_recv[k].astype(F32)).astype(BF16)
            z_copies[k] = remote(
                z_send.at[k], z_recv.at[k], z_ss.at[k], z_rs.at[k], {"dp": zz * inner + x}
            )
            z_copies[k].start()
    sums = sum_send[me]
    for m in range(1, dp_count):
        sum_copies[m - 1].wait_recv()
        sums = sums + sum_recv[m]
    inverse = lax.rsqrt(jnp.sum(jnp.where(eye, sums, 0.0), axis=1, keepdims=True) / width + EPS)
    for k in order[:-1]:
        z_copies[k].wait_recv()

    for lower in range(0, rows, ROW_CHUNK):
        rows_now = pl.ds(lower, ROW_CHUNK)
        value = total[rows_now]
        for k in order[:-1]:
            value = value + z_recv[k, rows_now].astype(F32)
        value = value * inverse[lower : lower + ROW_CHUNK]
        hid[me, rows_now] = jax.nn.gelu(value, approximate=True).astype(BF16)

    def forward(origin, sem_id):
        return remote(
            hid.at[origin * inner + x],
            hid.at[origin * inner + x],
            fx_ss.at[sem_id],
            fx_rs.at[sem_id],
            {"dp": z * inner + peer},
        )

    def expect(origin, sem_id):
        return remote(
            hid.at[origin * inner + peer],
            hid.at[origin * inner + peer],
            fx_ss.at[sem_id],
            fx_rs.at[sem_id],
            {"dp": z * inner + peer},
        )

    def hop(origin, target, sends, recvs, j):
        return remote(
            hid.at[origin * inner + x],
            hid.at[origin * inner + x],
            sends.at[j],
            recvs.at[j],
            {"dp": target * inner + x},
        )

    def landing(origin, sends, recvs, j):
        return remote(
            hid.at[origin * inner + x],
            hid.at[origin * inner + x],
            sends.at[j],
            recvs.at[j],
            {"dp": z * inner + peer},
        )

    def store(block):
        return pltpu.make_async_copy(hid.at[block], hid_out.at[block], out_sem.at[block])

    def part_copy(block):
        return remote(
            part_send.at[block],
            part_recv.at[block // group, member],
            part_ss.at[block],
            part_rs.at[(block // group) * group + member],
            place(lax.rem(block, group)),
        )

    def part_landing(block, off):
        source = lax.rem(member + off, group)
        return remote(
            part_send.at[block],
            part_recv.at[block // group, source],
            part_ss.at[block],
            part_rs.at[(block // group) * group + source],
            place(source),
        )

    def next_copy(block, off):
        return remote(
            x_next.at[block],
            x_next.at[block],
            xn_ss.at[(block // group) * group + off],
            xn_rs.at[block],
            place(lax.rem(member + off, group)),
        )

    slot = lax.rem(me, per_tensor)

    def state_copy(block):
        return remote(
            x_next.at[block],
            state_buf.at[slot],
            st_ss.at[block // group],
            st_rs.at[slot],
            {"section": layer, "dp": block, "tensor": me // per_tensor},
        )

    def state_local(block):
        return pltpu.make_async_copy(x_next.at[block], state_buf.at[slot], st_rs.at[slot])

    def finish(block):
        @pl.when(lax.rem(block, group) == member)
        def _():
            sum_now = part_send[block].astype(F32)
            for off in range(1, group):
                part_landing(block, off).wait_recv()
                sum_now = sum_now + part_recv[
                    block // group, lax.rem(member + off, group)
                ].astype(F32)
            x_next[block] = (x_ref[block].astype(F32) + sum_now).astype(BF16)
            if not is_last:
                for off in range(1, group):
                    next_copy(block, off).start()
            local = state_is_local(block)

            @pl.when(local)
            def _():
                state_local(block).start()

            @pl.when(jnp.logical_not(local))
            def _():
                state_copy(block).start()

    waiting = []

    def finish_oldest():
        valid, block = waiting.pop(0)
        if valid is None:
            finish(block)
        else:
            pl.when(valid)(lambda: finish(block))

    def use(block):
        store(block).start()
        part_send[block] = jnp.dot(
            hid[block], down_ref[...], preferred_element_type=F32
        ).astype(BF16)

        @pl.when(lax.rem(block, group) != member)
        def _():
            part_copy(block).start()

    def queue(valid, block):
        waiting.append((valid, block))
        if len(waiting) > 3:
            finish_oldest()

    last = outer - 1

    def start_hops(j):
        @pl.when((z - j >= 0) & (z < last))
        def _():
            hop(z - j, z + 1, up_ss, up_rs, j).start()

        @pl.when((z + j <= last) & (z > 0))
        def _():
            hop(z + j, z - 1, dn_ss, dn_rs, j).start()

    def use_peers(j):
        if j == 0:
            expect(z, 0).wait_recv()
            use(z * inner + peer)
            queue(None, z * inner + peer)
            return
        for valid, origin, sem_id in (
            (z - j >= 0, z - j, j),
            (z + j <= last, z + j, last + j),
        ):

            @pl.when(valid)
            def _():
                expect(origin, sem_id).wait_recv()
                use(origin * inner + peer)

            queue(valid, origin * inner + peer)

    start_hops(0)
    forward(z, 0).start()
    use(me)
    queue(None, me)
    for j in range(1, outer):
        above, below = z - j >= 0, z + j <= last

        @pl.when(above)
        def _():
            landing(z - j, up_ss, up_rs, j - 1).wait_recv()
            forward(z - j, j).start()

        @pl.when(below)
        def _():
            landing(z + j, dn_ss, dn_rs, j - 1).wait_recv()
            forward(z + j, last + j).start()

        if j < last:
            start_hops(j)
        for valid, origin in ((above, z - j), (below, z + j)):
            pl.when(valid)(lambda: use(origin * inner + x))
            queue(valid, origin * inner + x)
        use_peers(j - 1)
    use_peers(last)
    while waiting:
        finish_oldest()

    if not is_last:
        for block in range(dp_count):

            @pl.when(block % group != member)
            def _():
                next_copy(block, 0).wait_recv()

        pltpu.make_async_copy(x_next, x_out, end_sem.at[0]).start()

    @pl.when(core == layer)
    def _():
        stores = []
        for q in range(per_tensor):
            pltpu.make_async_copy(x_next.at[0], state_buf.at[q], st_rs.at[q]).wait()
            copy = pltpu.make_async_copy(
                state_buf.at[q],
                state_out.at[:, pl.ds(q * x_ref.shape[2], x_ref.shape[2])],
                end_sem.at[1 + q],
            )
            copy.start()
            stores.append(copy)
        for copy in stores:
            copy.wait()

    if not is_last:
        pltpu.make_async_copy(x_next, x_out, end_sem.at[0]).wait()
    for block in range(dp_count):

        @pl.when(block % group != member)
        def _():
            part_copy(block).wait_send()

    for i in range(owned):
        block = member + i * group
        if not is_last:
            for off in range(1, group):
                next_copy(block, off).wait_send()

        @pl.when(jnp.logical_not(state_is_local(block)))
        def _():
            state_copy(block).wait_send()

    for copy in list(x_copies.values()) + list(z_copies.values()) + sum_copies:
        copy.wait_send()
    forward(z, 0).wait_send()
    for j in range(last):

        @pl.when((z - j >= 0) & (z < last))
        def _():
            hop(z - j, z + 1, up_ss, up_rs, j).wait_send()

        @pl.when((z + j <= last) & (z > 0))
        def _():
            hop(z + j, z - 1, dn_ss, dn_rs, j).wait_send()

        @pl.when(z - 1 - j >= 0)
        def _():
            forward(z - 1 - j, 1 + j).wait_send()

        @pl.when(z + 1 + j <= last)
        def _():
            forward(z + 1 + j, outer + j).wait_send()

    for block in range(dp_count):
        store(block).wait()


def layer_step(layer, sizes, width, x, gain_row, up, down):
    sections, dp_count, tensors = sizes
    rows, slice_width = x.shape[1:]
    half = up.shape[1]
    inner = 2
    group = sections * tensors
    assert dp_count % inner == 0 and dp_count % group == 0
    outer = dp_count // inner
    per_tensor = dp_count // tensors
    is_last = layer == sections - 1
    dma = pltpu.SemaphoreType.DMA
    vmem = pl.BlockSpec(memory_space=pltpu.VMEM)
    hbm = pl.BlockSpec(memory_space=pl.ANY)
    wide = pltpu.VMEM((outer, rows, half), BF16)
    thin = pltpu.VMEM((dp_count, rows, slice_width), BF16)
    x_shape = x.shape if not is_last else (1, 8, 128)
    return pl.pallas_call(
        functools.partial(layer_kernel, sizes, inner, width, layer, is_last),
        name=f"layer{layer}",
        out_shape=(
            jax.ShapeDtypeStruct((dp_count, rows, half), BF16),
            jax.ShapeDtypeStruct(x_shape, BF16),
            jax.ShapeDtypeStruct((rows, per_tensor * slice_width), BF16),
        ),
        in_specs=[vmem] * 4,
        out_specs=(hbm, hbm, hbm),
        scratch_shapes=[
            thin,
            pltpu.VMEM((dp_count, 1, rows), F32),
            pltpu.VMEM((dp_count, 1, rows), F32),
            wide,
            wide,
            wide,
            wide,
            pltpu.VMEM((rows, half), F32),
            pltpu.VMEM((dp_count, rows, half), BF16),
            thin,
            pltpu.VMEM((dp_count // group, group, rows, slice_width), BF16),
            thin,
            pltpu.VMEM((per_tensor, rows, slice_width), BF16),
        ]
        + [dma((dp_count,))] * 2
        + [dma((outer,))] * 8
        + [dma((2 * outer,))] * 2
        + [dma((dp_count,))]
        + [dma((dp_count,))] * 4
        + [dma((dp_count // group,)), dma((per_tensor,)), dma((1 + per_tensor,))],
        compiler_params=pltpu.CompilerParams(collective_id=layer, has_side_effects=True),
    )(x, gain_row, up, down)


def body(tokens, gain, w_up, w_down, cotangent):
    core = lax.axis_index("section")
    layers = lax.axis_size("section")
    assert layers == 2
    dp_id = lax.axis_index("dp")
    dp_count = lax.axis_size("dp")
    tensor_count = lax.axis_size("tensor")
    rows, own_width = tokens.shape
    width = own_width * tensor_count
    slice_width = width // dp_count
    hidden_width = w_up.shape[2]
    half = hidden_width // layers
    other = 1 - core
    all_rows = rows * dp_count

    def swap(array):
        return lax.ppermute(array, "section", [(0, 1), (1, 0)])

    def both(own, got):
        return (jnp.where(core == 0, own, got), jnp.where(core == 0, got, own))

    cot_mine = lax.all_to_all(cotangent[0], "dp", split_axis=1, concat_axis=0, tiled=True)

    half_rows = rows // layers
    tok_half = lax.dynamic_slice_in_dim(tokens, core * half_rows, half_rows, 0)
    tok_full = lax.all_gather(tok_half, "tensor", axis=1, tiled=True)
    x_half = lax.all_to_all(tok_full, "dp", split_axis=1, concat_axis=0, tiled=True)
    x_a, x_b = both(x_half, swap(x_half))
    x = jnp.concatenate(
        [
            x_a.reshape(dp_count, half_rows, slice_width),
            x_b.reshape(dp_count, half_rows, slice_width),
        ],
        axis=1,
    ).reshape(all_rows, slice_width)

    gain_all = lax.all_gather(gain, "tensor", axis=1, tiled=True)
    gain_own = lax.dynamic_slice_in_dim(gain_all, dp_id * slice_width, slice_width, 1)
    gains = both(gain_own, swap(gain_own))

    up_parts = both(
        lax.dynamic_slice_in_dim(w_up[0], core * half, half, 1),
        swap(lax.dynamic_slice_in_dim(w_up[0], other * half, half, 1)),
    )
    down_parts = both(
        lax.dynamic_slice_in_dim(w_down[0], core * half, half, 0),
        swap(lax.dynamic_slice_in_dim(w_down[0], other * half, half, 0)),
    )

    states = []
    hiddens = []
    sizes = (layers, dp_count, tensor_count)
    x = x.reshape(dp_count, rows, slice_width)
    for layer in range(layers):
        hidden, x, state = layer_step(
            layer, sizes, width, x, gains[layer], up_parts[layer], down_parts[layer]
        )
        hiddens.append(hidden.reshape(all_rows, half))
        states.append(state)
    state = jnp.where(core == 0, states[0], states[1])

    hid_keep = jnp.where(core == 0, hiddens[0], hiddens[1])
    hid_got = swap(jnp.where(core == 0, hiddens[1], hiddens[0]))
    hid_parts = both(hid_keep, hid_got)
    hidden_whole = jnp.concatenate(hid_parts, axis=1)
    grad = lax.dot_general(
        hidden_whole, cot_mine, (((0,), (0,)), ((), ())), preferred_element_type=F32
    ).astype(BF16)
    return (state[None], grad[None])


def solution(mesh):
    placed = (
        P("dp", "tensor"),
        P("section", "tensor"),
        P("section", "dp", "tensor"),
        P("section", "tensor", "dp"),
        P("section", "dp", None),
    )
    return jax.shard_map(
        body,
        mesh=mesh,
        in_specs=placed,
        out_specs=(P("section", "dp", "tensor"), P("section", "tensor", "dp")),
        check_vma=False,
    )
```

```python
import functools

import jax
import jax.numpy as jnp
from jax import lax
from jax.experimental import pallas as pl
from jax.experimental.pallas import tpu as pltpu
from jax.sharding import PartitionSpec as P

EPS = 1e-06
F32 = jnp.float32
BF16 = jnp.bfloat16


MESH = pl.DeviceIdType.MESH
ROW_CHUNK = 16


def far_first(count):
    return sorted(range(1, count), key=lambda k: abs(2 * k - count)) + [0]


def remote(src, dst, send_sem, recv_sem, target):
    return pltpu.make_async_remote_copy(
        src_ref=src,
        dst_ref=dst,
        send_sem=send_sem,
        recv_sem=recv_sem,
        device_id=target,
        device_id_type=MESH,
    )


def layer_kernel(
    sizes,
    inner,
    width,
    layer,
    is_last,
    x_ref,
    gain_ref,
    up_ref,
    down_ref,
    hid_out,
    x_out,
    state_out,
    scaled,
    sum_send,
    sum_recv,
    x_send,
    x_recv,
    z_send,
    z_recv,
    total,
    hid,
    part_send,
    part_recv,
    x_next,
    state_buf,
    sum_ss,
    sum_rs,
    x_ss,
    x_rs,
    z_ss,
    z_rs,
    up_ss,
    up_rs,
    dn_ss,
    dn_rs,
    fx_ss,
    fx_rs,
    out_sem,
    part_ss,
    part_rs,
    xn_ss,
    xn_rs,
    st_ss,
    st_rs,
    end_sem,
):
    sections, dp_count, tensors = sizes
    outer = dp_count // inner
    group = sections * tensors
    owned = dp_count // group
    per_tensor = dp_count // tensors
    core = lax.axis_index("section")
    tensor = lax.axis_index("tensor")
    member = tensor * sections + core
    me = lax.axis_index("dp")
    z = me // inner
    x = lax.rem(me, inner)
    peer = 1 - x
    rows = x_ref.shape[1]

    barrier = pltpu.get_barrier_semaphore()
    for m in range(1, dp_count):
        pl.semaphore_signal(
            barrier, inc=1, device_id={"dp": lax.rem(me + m, dp_count)}, device_id_type=MESH
        )

    def place(index):
        return {"section": lax.rem(index, sections), "tensor": index // sections}

    for off in range(1, group):
        pl.semaphore_signal(
            barrier, inc=1, device_id=place(lax.rem(member + off, group)), device_id_type=MESH
        )
    giver = lax.rem(me, group)
    for q in range(per_tensor):
        source = tensor * per_tensor + q
        apart = (giver != member) | (source != me)

        @pl.when((core == layer) & apart)
        def _():
            pl.semaphore_signal(
                barrier, inc=1, device_id={"dp": source, **place(giver)}, device_id_type=MESH
            )

    def state_is_local(block):
        return (core == layer) & (block == me) & (tensor == me // per_tensor)

    arrivals = dp_count - 1 + group - 1 + owned
    for i in range(owned):
        arrivals = arrivals - state_is_local(member + i * group).astype(jnp.int32)
    pl.semaphore_wait(barrier, arrivals)

    row_id = lax.broadcasted_iota(jnp.int32, (rows, rows), 0)
    col_id = lax.broadcasted_iota(jnp.int32, (rows, rows), 1)
    eye = row_id == col_id
    gain_f = gain_ref[...].astype(F32)

    def prepare(block, _):
        values = x_ref[block].astype(F32)
        scaled[block] = (values * gain_f).astype(BF16)
        column = jnp.sum(values * values, axis=1, keepdims=True)
        sum_send[block] = jnp.sum(jnp.where(eye, column, 0.0), axis=0, keepdims=True)
        return 0

    lax.fori_loop(0, dp_count, prepare, 0)

    order = far_first(outer)
    x_copies = {}
    for k in order:
        zz = lax.rem(z + k, outer)
        x_send[k] = jnp.dot(
            scaled[zz * inner + peer], up_ref[...], preferred_element_type=F32
        ).astype(BF16)
        x_copies[k] = remote(
            x_send.at[k], x_recv.at[k], x_ss.at[k], x_rs.at[k], {"dp": z * inner + peer}
        )
        x_copies[k].start()
    sum_copies = []
    for m in range(1, dp_count):
        target = lax.rem(me + m, dp_count)
        copy = remote(
            sum_send.at[target], sum_recv.at[m], sum_ss.at[m], sum_rs.at[m], {"dp": target}
        )
        copy.start()
        sum_copies.append(copy)
    z_copies = {}
    for k in order:
        zz = lax.rem(z + k, outer)
        mine = jnp.dot(scaled[zz * inner + x], up_ref[...], preferred_element_type=F32)
        x_copies[k].wait_recv()
        if k == 0:
            total[...] = mine + x_recv[k].astype(F32)
        else:
            z_send[k] = (mine + x_recv[k].astype(F32)).astype(BF16)
            z_copies[k] = remote(
                z_send.at[k], z_recv.at[k], z_ss.at[k], z_rs.at[k], {"dp": zz * inner + x}
            )
            z_copies[k].start()
    sums = sum_send[me]
    for m in range(1, dp_count):
        sum_copies[m - 1].wait_recv()
        sums = sums + sum_recv[m]
    inverse = lax.rsqrt(jnp.sum(jnp.where(eye, sums, 0.0), axis=1, keepdims=True) / width + EPS)
    for k in order[:-1]:
        z_copies[k].wait_recv()

    for lower in range(0, rows, ROW_CHUNK):
        rows_now = pl.ds(lower, ROW_CHUNK)
        value = total[rows_now]
        for k in order[:-1]:
            value = value + z_recv[k, rows_now].astype(F32)
        value = value * inverse[lower : lower + ROW_CHUNK]
        hid[me, rows_now] = jax.nn.gelu(value, approximate=True).astype(BF16)

    def forward(origin, sem_id):
        return remote(
            hid.at[origin * inner + x],
            hid.at[origin * inner + x],
            fx_ss.at[sem_id],
            fx_rs.at[sem_id],
            {"dp": z * inner + peer},
        )

    def expect(origin, sem_id):
        return remote(
            hid.at[origin * inner + peer],
            hid.at[origin * inner + peer],
            fx_ss.at[sem_id],
            fx_rs.at[sem_id],
            {"dp": z * inner + peer},
        )

    def hop(origin, target, sends, recvs, j):
        return remote(
            hid.at[origin * inner + x],
            hid.at[origin * inner + x],
            sends.at[j],
            recvs.at[j],
            {"dp": target * inner + x},
        )

    def landing(origin, sends, recvs, j):
        return remote(
            hid.at[origin * inner + x],
            hid.at[origin * inner + x],
            sends.at[j],
            recvs.at[j],
            {"dp": z * inner + peer},
        )

    def store(block):
        return pltpu.make_async_copy(hid.at[block], hid_out.at[block], out_sem.at[block])

    def part_copy(block):
        return remote(
            part_send.at[block],
            part_recv.at[block // group, member],
            part_ss.at[block],
            part_rs.at[(block // group) * group + member],
            place(lax.rem(block, group)),
        )

    def part_landing(block, off):
        source = lax.rem(member + off, group)
        return remote(
            part_send.at[block],
            part_recv.at[block // group, source],
            part_ss.at[block],
            part_rs.at[(block // group) * group + source],
            place(source),
        )

    def next_copy(block, off):
        return remote(
            x_next.at[block],
            x_next.at[block],
            xn_ss.at[(block // group) * group + off],
            xn_rs.at[block],
            place(lax.rem(member + off, group)),
        )

    slot = lax.rem(me, per_tensor)

    def state_copy(block):
        return remote(
            x_next.at[block],
            state_buf.at[slot],
            st_ss.at[block // group],
            st_rs.at[slot],
            {"section": layer, "dp": block, "tensor": me // per_tensor},
        )

    def state_local(block):
        return pltpu.make_async_copy(x_next.at[block], state_buf.at[slot], st_rs.at[slot])

    def finish(block):
        @pl.when(lax.rem(block, group) == member)
        def _():
            sum_now = part_send[block].astype(F32)
            for off in range(1, group):
                part_landing(block, off).wait_recv()
                sum_now = sum_now + part_recv[
                    block // group, lax.rem(member + off, group)
                ].astype(F32)
            x_next[block] = (x_ref[block].astype(F32) + sum_now).astype(BF16)
            if not is_last:
                for off in range(1, group):
                    next_copy(block, off).start()
            local = state_is_local(block)

            @pl.when(local)
            def _():
                state_local(block).start()

            @pl.when(jnp.logical_not(local))
            def _():
                state_copy(block).start()

    waiting = []

    def finish_oldest():
        valid, block = waiting.pop(0)
        if valid is None:
            finish(block)
        else:
            pl.when(valid)(lambda: finish(block))

    def use(block):
        store(block).start()
        part_send[block] = jnp.dot(
            hid[block], down_ref[...], preferred_element_type=F32
        ).astype(BF16)

        @pl.when(lax.rem(block, group) != member)
        def _():
            part_copy(block).start()

    def queue(valid, block):
        waiting.append((valid, block))
        if len(waiting) > 3:
            finish_oldest()

    last = outer - 1

    def start_hops(j):
        @pl.when((z - j >= 0) & (z < last))
        def _():
            hop(z - j, z + 1, up_ss, up_rs, j).start()

        @pl.when((z + j <= last) & (z > 0))
        def _():
            hop(z + j, z - 1, dn_ss, dn_rs, j).start()

    def use_peers(j):
        if j == 0:
            expect(z, 0).wait_recv()
            use(z * inner + peer)
            queue(None, z * inner + peer)
            return
        for valid, origin, sem_id in (
            (z - j >= 0, z - j, j),
            (z + j <= last, z + j, last + j),
        ):

            @pl.when(valid)
            def _():
                expect(origin, sem_id).wait_recv()
                use(origin * inner + peer)

            queue(valid, origin * inner + peer)

    start_hops(0)
    forward(z, 0).start()
    use(me)
    queue(None, me)
    for j in range(1, outer):
        above, below = z - j >= 0, z + j <= last

        @pl.when(above)
        def _():
            landing(z - j, up_ss, up_rs, j - 1).wait_recv()
            forward(z - j, j).start()

        @pl.when(below)
        def _():
            landing(z + j, dn_ss, dn_rs, j - 1).wait_recv()
            forward(z + j, last + j).start()

        if j < last:
            start_hops(j)
        for valid, origin in ((above, z - j), (below, z + j)):
            pl.when(valid)(lambda: use(origin * inner + x))
            queue(valid, origin * inner + x)
        use_peers(j - 1)
    use_peers(last)
    while waiting:
        finish_oldest()

    if not is_last:
        for block in range(dp_count):

            @pl.when(block % group != member)
            def _():
                next_copy(block, 0).wait_recv()

        pltpu.make_async_copy(x_next, x_out, end_sem.at[0]).start()

    @pl.when(core == layer)
    def _():
        stores = []
        for q in range(per_tensor):
            pltpu.make_async_copy(x_next.at[0], state_buf.at[q], st_rs.at[q]).wait()
            copy = pltpu.make_async_copy(
                state_buf.at[q],
                state_out.at[:, pl.ds(q * x_ref.shape[2], x_ref.shape[2])],
                end_sem.at[1 + q],
            )
            copy.start()
            stores.append(copy)
        for copy in stores:
            copy.wait()

    if not is_last:
        pltpu.make_async_copy(x_next, x_out, end_sem.at[0]).wait()
    for block in range(dp_count):

        @pl.when(block % group != member)
        def _():
            part_copy(block).wait_send()

    for i in range(owned):
        block = member + i * group
        if not is_last:
            for off in range(1, group):
                next_copy(block, off).wait_send()

        @pl.when(jnp.logical_not(state_is_local(block)))
        def _():
            state_copy(block).wait_send()

    for copy in list(x_copies.values()) + list(z_copies.values()) + sum_copies:
        copy.wait_send()
    forward(z, 0).wait_send()
    for j in range(last):

        @pl.when((z - j >= 0) & (z < last))
        def _():
            hop(z - j, z + 1, up_ss, up_rs, j).wait_send()

        @pl.when((z + j <= last) & (z > 0))
        def _():
            hop(z + j, z - 1, dn_ss, dn_rs, j).wait_send()

        @pl.when(z - 1 - j >= 0)
        def _():
            forward(z - 1 - j, 1 + j).wait_send()

        @pl.when(z + 1 + j <= last)
        def _():
            forward(z + 1 + j, outer + j).wait_send()

    for block in range(dp_count):
        store(block).wait()


def layer_step(layer, sizes, width, x, gain_row, up, down):
    sections, dp_count, tensors = sizes
    rows, slice_width = x.shape[1:]
    half = up.shape[1]
    inner = 2
    group = sections * tensors
    assert dp_count % inner == 0 and dp_count % group == 0
    outer = dp_count // inner
    per_tensor = dp_count // tensors
    is_last = layer == sections - 1
    dma = pltpu.SemaphoreType.DMA
    vmem = pl.BlockSpec(memory_space=pltpu.VMEM)
    hbm = pl.BlockSpec(memory_space=pl.ANY)
    wide = pltpu.VMEM((outer, rows, half), BF16)
    thin = pltpu.VMEM((dp_count, rows, slice_width), BF16)
    x_shape = x.shape if not is_last else (1, 8, 128)
    return pl.pallas_call(
        functools.partial(layer_kernel, sizes, inner, width, layer, is_last),
        name=f"layer{layer}",
        out_shape=(
            jax.ShapeDtypeStruct((dp_count, rows, half), BF16),
            jax.ShapeDtypeStruct(x_shape, BF16),
            jax.ShapeDtypeStruct((rows, per_tensor * slice_width), BF16),
        ),
        in_specs=[vmem] * 4,
        out_specs=(hbm, hbm, hbm),
        scratch_shapes=[
            thin,
            pltpu.VMEM((dp_count, 1, rows), F32),
            pltpu.VMEM((dp_count, 1, rows), F32),
            wide,
            wide,
            wide,
            wide,
            pltpu.VMEM((rows, half), F32),
            pltpu.VMEM((dp_count, rows, half), BF16),
            thin,
            pltpu.VMEM((dp_count // group, group, rows, slice_width), BF16),
            thin,
            pltpu.VMEM((per_tensor, rows, slice_width), BF16),
        ]
        + [dma((dp_count,))] * 2
        + [dma((outer,))] * 8
        + [dma((2 * outer,))] * 2
        + [dma((dp_count,))]
        + [dma((dp_count,))] * 4
        + [dma((dp_count // group,)), dma((per_tensor,)), dma((1 + per_tensor,))],
        compiler_params=pltpu.CompilerParams(collective_id=layer, has_side_effects=True),
    )(x, gain_row, up, down)


def front_kernel(
    sizes,
    tok_ref,
    gain_ref,
    up_ref,
    down_ref,
    cot_ref,
    x_out,
    gain_out0,
    gain_out1,
    up_out0,
    up_out1,
    down_out0,
    down_out1,
    cot_out,
    x_buf,
    gain_buf,
    up_buf,
    down_buf,
    cot_buf,
    tok_ss,
    tok_rs,
    tf_ss,
    tf_rs,
    cot_ss,
    cot_rs,
    cy_ss,
    cy_rs,
    gain_ss,
    gain_rs,
    w_ss,
    w_rs,
    own_sem,
    end_sem,
):
    sections, dp_count, tensors = sizes
    group = sections * tensors
    per_tensor = dp_count // tensors
    core = lax.axis_index("section")
    tensor = lax.axis_index("tensor")
    me = lax.axis_index("dp")
    other = 1 - core
    member = tensor * sections + core
    rows, slice_width = x_buf.shape[1:]
    half = up_buf.shape[2]
    half_rows = rows // sections
    part_rows = rows // tensors

    def place(index):
        return {"section": lax.rem(index, sections), "tensor": index // sections}

    barrier = pltpu.get_barrier_semaphore()

    def greet(target):
        pl.semaphore_signal(barrier, inc=1, device_id=target, device_id_type=MESH)

    for m in range(1, dp_count):
        greet({"dp": lax.rem(me + m, dp_count)})
    for off in range(1, group):
        greet(place(lax.rem(member + off, group)))
    feature_home = me // per_tensor
    at_home = feature_home == tensor
    for source in range(dp_count):

        @pl.when(jnp.logical_not(at_home & (me == source)))
        def _():
            greet({"dp": source, "tensor": feature_home})

    self_send = at_home.astype(jnp.int32)
    pl.semaphore_wait(barrier, dp_count - 1 + group - 1 + per_tensor * tensors - self_send)

    my_half = pl.ds(pl.multiple_of(core * half_rows, half_rows), half_rows)
    my_part = pl.ds(pl.multiple_of(tensor * part_rows, part_rows), part_rows)

    def columns(index, size):
        return pl.ds(pl.multiple_of(index * size, size), size)

    def token_copy(q, tt):
        return remote(
            tok_ref.at[my_half, pl.ds(q * slice_width, slice_width)],
            x_buf.at[me, my_half],
            tok_ss.at[q * tensors + tt],
            tok_rs.at[me],
            {"dp": tensor * per_tensor + q, "tensor": tt},
        )

    def token_local(q):
        return pltpu.make_async_copy(
            tok_ref.at[my_half, pl.ds(q * slice_width, slice_width)],
            x_buf.at[me, my_half],
            tok_rs.at[me],
        )

    def is_self(q, tt):
        return (tensor * per_tensor + q == me) & (tensor == tt)

    for q in range(per_tensor):
        for tt in range(tensors):
            local = is_self(q, tt)

            @pl.when(local)
            def _():
                token_local(q).start()

            @pl.when(jnp.logical_not(local))
            def _():
                token_copy(q, tt).start()

    def gain_copy(off):
        return remote(
            gain_ref.at[:, columns(lax.rem(me, per_tensor), slice_width)],
            gain_buf.at[core],
            gain_ss.at[off],
            gain_rs.at[core],
            place(lax.rem(member + off, group)),
        )

    gain_local = pltpu.make_async_copy(
        gain_ref.at[:, columns(lax.rem(me, per_tensor), slice_width)],
        gain_buf.at[core],
        gain_rs.at[core],
    )

    @pl.when(at_home)
    def _():
        gain_local.start()
        for off in range(1, group):
            gain_copy(off).start()

    def up_half(index):
        if up_ref.shape[0] == sections:
            return up_ref.at[index]
        return up_ref.at[0, :, columns(index, half)]

    give_up = remote(
        up_half(other),
        up_buf.at[core],
        w_ss.at[0],
        w_rs.at[0],
        {"section": other},
    )
    give_up.start()
    own_up = pltpu.make_async_copy(
        up_half(core), up_buf.at[core], own_sem.at[0]
    )
    own_up.start()

    cot_copies = []
    for m in range(1, dp_count):
        target = lax.rem(me + m, dp_count)
        copy = remote(
            cot_ref.at[0, my_part, columns(target, slice_width)],
            cot_buf.at[me, my_part],
            cot_ss.at[m],
            cot_rs.at[m],
            {"dp": target},
        )
        copy.start()
        cot_copies.append(copy)
    cot_local = pltpu.make_async_copy(
        cot_ref.at[0, my_part, columns(me, slice_width)], cot_buf.at[me, my_part], own_sem.at[2]
    )
    cot_local.start()

    give_down = remote(
        down_ref.at[0, columns(other, half), :],
        down_buf.at[core],
        w_ss.at[1],
        w_rs.at[1],
        {"section": other},
    )
    give_down.start()
    own_down = pltpu.make_async_copy(
        down_ref.at[0, columns(core, half), :], down_buf.at[core], own_sem.at[1]
    )
    own_down.start()

    def token_forward(source):
        return remote(
            x_buf.at[source, my_half],
            x_buf.at[source, my_half],
            tf_ss.at[source],
            tf_rs.at[source],
            {"section": other},
        )

    their_half = columns(other, half_rows)
    for source in range(dp_count):
        pltpu.make_async_copy(
            x_buf.at[source, my_half], x_buf.at[source, my_half], tok_rs.at[source]
        ).wait()
        token_forward(source).start()

    ends = []

    def put(src, dst):
        copy = pltpu.make_async_copy(src, dst, end_sem.at[len(ends)])
        copy.start()
        ends.append(copy)

    own_up.wait()
    give_up.wait_recv()
    put(up_buf.at[0], up_out0)
    put(up_buf.at[1], up_out1)
    own_down.wait()
    give_down.wait_recv()
    put(down_buf.at[0], down_out0)
    put(down_buf.at[1], down_out1)
    for layer in range(sections):
        pltpu.make_async_copy(
            gain_buf.at[layer], gain_buf.at[layer], gain_rs.at[layer]
        ).wait()
    put(gain_buf.at[0], gain_out0)
    put(gain_buf.at[1], gain_out1)

    def cot_share(m, off):
        source = lax.rem(me + dp_count - m, dp_count)
        return remote(
            cot_buf.at[source, my_part],
            cot_buf.at[source, my_part],
            cy_ss.at[m * tensors + off],
            cy_rs.at[m * tensors + off],
            {"tensor": lax.rem(tensor + off, tensors)},
        )

    for m in range(dp_count):
        if m == 0:
            cot_local.wait()
        else:
            cot_copies[m - 1].wait_recv()
        for off in range(1, tensors):
            cot_share(m, off).start()

    for source in range(dp_count):
        token_forward(source).wait_recv()
    put(x_buf, x_out)
    for m in range(dp_count):
        for off in range(1, tensors):
            cot_share(m, off).wait_recv()
    put(cot_buf, cot_out)

    for q in range(per_tensor):
        for tt in range(tensors):

            @pl.when(jnp.logical_not(is_self(q, tt)))
            def _():
                token_copy(q, tt).wait_send()

    @pl.when(at_home)
    def _():
        for off in range(1, group):
            gain_copy(off).wait_send()

    give_up.wait_send()
    give_down.wait_send()
    for copy in cot_copies:
        copy.wait_send()
    for source in range(dp_count):
        token_forward(source).wait_send()
    for m in range(dp_count):
        for off in range(1, tensors):
            cot_share(m, off).wait_send()
    for copy in ends:
        copy.wait()


def front(sizes, tokens, gain, w_up, w_down, cotangent):
    sections, dp_count, tensors = sizes
    assert sections == 2
    group = sections * tensors
    per_tensor = dp_count // tensors
    rows, own_width = tokens.shape
    slice_width = own_width // per_tensor
    depth = w_up.shape[1]
    half = w_up.shape[2] // sections
    dma = pltpu.SemaphoreType.DMA
    hbm = pl.BlockSpec(memory_space=pl.ANY)
    if half % 128:
        w_up = w_up[0].reshape(depth, sections, half).transpose(1, 0, 2)

    def shape(*dims, dtype=BF16):
        return jax.ShapeDtypeStruct(dims, dtype)

    return pl.pallas_call(
        functools.partial(front_kernel, sizes),
        name="front",
        out_shape=(
            shape(dp_count, rows, slice_width),
            shape(1, slice_width, dtype=F32),
            shape(1, slice_width, dtype=F32),
            shape(depth, half),
            shape(depth, half),
            shape(half, slice_width),
            shape(half, slice_width),
            shape(dp_count, rows, slice_width),
        ),
        in_specs=[hbm] * 5,
        out_specs=(hbm,) * 8,
        scratch_shapes=[
            pltpu.VMEM((dp_count, rows, slice_width), BF16),
            pltpu.VMEM((sections, 1, slice_width), F32),
            pltpu.VMEM((sections, depth, half), BF16),
            pltpu.VMEM((sections, half, slice_width), BF16),
            pltpu.VMEM((dp_count, rows, slice_width), BF16),
            dma((dp_count,)),
            dma((dp_count,)),
            dma((dp_count,)),
            dma((dp_count,)),
            dma((dp_count,)),
            dma((dp_count,)),
            dma((dp_count * tensors,)),
            dma((dp_count * tensors,)),
            dma((group,)),
            dma((sections,)),
            dma((2,)),
            dma((2,)),
            dma((3,)),
            dma((8,)),
        ],
        compiler_params=pltpu.CompilerParams(collective_id=sections, has_side_effects=True),
    )(tokens, gain.astype(F32), w_up, w_down, cotangent)


def body(tokens, gain, w_up, w_down, cotangent):
    core = lax.axis_index("section")
    layers = lax.axis_size("section")
    dp_count = lax.axis_size("dp")
    tensor_count = lax.axis_size("tensor")
    rows, own_width = tokens.shape
    width = own_width * tensor_count
    half = w_up.shape[2] // layers
    all_rows = rows * dp_count
    sizes = (layers, dp_count, tensor_count)

    def swap(array):
        return lax.ppermute(array, "section", [(0, 1), (1, 0)])

    def both(own, got):
        return (jnp.where(core == 0, own, got), jnp.where(core == 0, got, own))

    x, *rest = front(sizes, tokens, gain, w_up, w_down, cotangent)
    gains, up_parts, down_parts = rest[0:2], rest[2:4], rest[4:6]
    cot_mine = rest[6].reshape(all_rows, -1)

    states = []
    hiddens = []
    for layer in range(layers):
        hidden, x, state = layer_step(
            layer, sizes, width, x, gains[layer], up_parts[layer], down_parts[layer]
        )
        hiddens.append(hidden.reshape(all_rows, half))
        states.append(state)
    state = jnp.where(core == 0, states[0], states[1])

    hid_keep = jnp.where(core == 0, hiddens[0], hiddens[1])
    hid_got = swap(jnp.where(core == 0, hiddens[1], hiddens[0]))
    hid_parts = both(hid_keep, hid_got)
    hidden_whole = jnp.concatenate(hid_parts, axis=1)
    grad = lax.dot_general(
        hidden_whole, cot_mine, (((0,), (0,)), ((), ())), preferred_element_type=F32
    ).astype(BF16)
    return (state[None], grad[None])


def solution(mesh):
    placed = (
        P("dp", "tensor"),
        P("section", "tensor"),
        P("section", "dp", "tensor"),
        P("section", "tensor", "dp"),
        P("section", "dp", None),
    )
    return jax.shard_map(
        body,
        mesh=mesh,
        in_specs=placed,
        out_specs=(P("section", "dp", "tensor"), P("section", "tensor", "dp")),
        check_vma=False,
    )
```

```python
import functools

import jax
import jax.numpy as jnp
from jax import lax
from jax.experimental import pallas as pl
from jax.experimental.pallas import tpu as pltpu
from jax.sharding import PartitionSpec as P

EPS = 1e-06
F32 = jnp.float32
BF16 = jnp.bfloat16


MESH = pl.DeviceIdType.MESH
ROW_CHUNK = 16


def far_first(count):
    return sorted(range(1, count), key=lambda k: abs(2 * k - count)) + [0]


def remote(src, dst, send_sem, recv_sem, target):
    return pltpu.make_async_remote_copy(
        src_ref=src,
        dst_ref=dst,
        send_sem=send_sem,
        recv_sem=recv_sem,
        device_id=target,
        device_id_type=MESH,
    )


def layer_kernel(
    sizes,
    inner,
    width,
    layer,
    is_last,
    x_ref,
    gain_ref,
    up_ref,
    down_ref,
    hid_out,
    x_out,
    state_out,
    scaled,
    sum_send,
    sum_recv,
    x_send,
    x_recv,
    z_send,
    z_recv,
    total,
    hid,
    part_send,
    part_recv,
    x_next,
    state_buf,
    sum_ss,
    sum_rs,
    x_ss,
    x_rs,
    z_ss,
    z_rs,
    up_ss,
    up_rs,
    dn_ss,
    dn_rs,
    fx_ss,
    fx_rs,
    out_sem,
    part_ss,
    part_rs,
    xn_ss,
    xn_rs,
    st_ss,
    st_rs,
    end_sem,
):
    sections, dp_count, tensors = sizes
    outer = dp_count // inner
    group = sections * tensors
    owned = dp_count // group
    per_tensor = dp_count // tensors
    core = lax.axis_index("section")
    tensor = lax.axis_index("tensor")
    member = tensor * sections + core
    me = lax.axis_index("dp")
    z = me // inner
    x = lax.rem(me, inner)
    peer = 1 - x
    rows = x_ref.shape[1]

    barrier = pltpu.get_barrier_semaphore()
    for m in range(1, dp_count):
        pl.semaphore_signal(
            barrier, inc=1, device_id={"dp": lax.rem(me + m, dp_count)}, device_id_type=MESH
        )

    def place(index):
        return {"section": lax.rem(index, sections), "tensor": index // sections}

    for off in range(1, group):
        pl.semaphore_signal(
            barrier, inc=1, device_id=place(lax.rem(member + off, group)), device_id_type=MESH
        )
    giver = lax.rem(me, group)
    for q in range(per_tensor):
        source = tensor * per_tensor + q
        apart = (giver != member) | (source != me)

        @pl.when((core == layer) & apart)
        def _():
            pl.semaphore_signal(
                barrier, inc=1, device_id={"dp": source, **place(giver)}, device_id_type=MESH
            )

    def state_is_local(block):
        return (core == layer) & (block == me) & (tensor == me // per_tensor)

    arrivals = dp_count - 1 + group - 1 + owned
    for i in range(owned):
        arrivals = arrivals - state_is_local(member + i * group).astype(jnp.int32)
    pl.semaphore_wait(barrier, arrivals)

    row_id = lax.broadcasted_iota(jnp.int32, (rows, rows), 0)
    col_id = lax.broadcasted_iota(jnp.int32, (rows, rows), 1)
    eye = row_id == col_id
    gain_f = gain_ref[...].astype(F32)

    def prepare(block, _):
        values = x_ref[block].astype(F32)
        scaled[block] = (values * gain_f).astype(BF16)
        column = jnp.sum(values * values, axis=1, keepdims=True)
        sum_send[block] = jnp.sum(jnp.where(eye, column, 0.0), axis=0, keepdims=True)
        return 0

    lax.fori_loop(0, dp_count, prepare, 0)

    order = far_first(outer)
    x_copies = {}
    for k in order:
        zz = lax.rem(z + k, outer)
        x_send[k] = jnp.dot(
            scaled[zz * inner + peer], up_ref[...], preferred_element_type=F32
        ).astype(BF16)
        x_copies[k] = remote(
            x_send.at[k], x_recv.at[k], x_ss.at[k], x_rs.at[k], {"dp": z * inner + peer}
        )
        x_copies[k].start()
    sum_copies = []
    for m in range(1, dp_count):
        target = lax.rem(me + m, dp_count)
        copy = remote(
            sum_send.at[target], sum_recv.at[m], sum_ss.at[m], sum_rs.at[m], {"dp": target}
        )
        copy.start()
        sum_copies.append(copy)
    z_copies = {}
    for k in order:
        zz = lax.rem(z + k, outer)
        mine = jnp.dot(scaled[zz * inner + x], up_ref[...], preferred_element_type=F32)
        x_copies[k].wait_recv()
        if k == 0:
            total[...] = mine + x_recv[k].astype(F32)
        else:
            z_send[k] = (mine + x_recv[k].astype(F32)).astype(BF16)
            z_copies[k] = remote(
                z_send.at[k], z_recv.at[k], z_ss.at[k], z_rs.at[k], {"dp": zz * inner + x}
            )
            z_copies[k].start()
    sums = sum_send[me]
    for m in range(1, dp_count):
        sum_copies[m - 1].wait_recv()
        sums = sums + sum_recv[m]
    inverse = lax.rsqrt(jnp.sum(jnp.where(eye, sums, 0.0), axis=1, keepdims=True) / width + EPS)
    for k in order[:-1]:
        z_copies[k].wait_recv()

    for lower in range(0, rows, ROW_CHUNK):
        rows_now = pl.ds(lower, ROW_CHUNK)
        value = total[rows_now]
        for k in order[:-1]:
            value = value + z_recv[k, rows_now].astype(F32)
        value = value * inverse[lower : lower + ROW_CHUNK]
        hid[me, rows_now] = jax.nn.gelu(value, approximate=True).astype(BF16)

    def forward(origin, sem_id):
        return remote(
            hid.at[origin * inner + x],
            hid.at[origin * inner + x],
            fx_ss.at[sem_id],
            fx_rs.at[sem_id],
            {"dp": z * inner + peer},
        )

    def expect(origin, sem_id):
        return remote(
            hid.at[origin * inner + peer],
            hid.at[origin * inner + peer],
            fx_ss.at[sem_id],
            fx_rs.at[sem_id],
            {"dp": z * inner + peer},
        )

    def hop(origin, target, sends, recvs, j):
        return remote(
            hid.at[origin * inner + x],
            hid.at[origin * inner + x],
            sends.at[j],
            recvs.at[j],
            {"dp": target * inner + x},
        )

    def landing(origin, sends, recvs, j):
        return remote(
            hid.at[origin * inner + x],
            hid.at[origin * inner + x],
            sends.at[j],
            recvs.at[j],
            {"dp": z * inner + peer},
        )

    def store(block):
        return pltpu.make_async_copy(hid.at[block], hid_out.at[block], out_sem.at[block])

    def part_copy(block):
        return remote(
            part_send.at[block],
            part_recv.at[block // group, member],
            part_ss.at[block],
            part_rs.at[(block // group) * group + member],
            place(lax.rem(block, group)),
        )

    def part_landing(block, off):
        source = lax.rem(member + off, group)
        return remote(
            part_send.at[block],
            part_recv.at[block // group, source],
            part_ss.at[block],
            part_rs.at[(block // group) * group + source],
            place(source),
        )

    def next_copy(block, off):
        return remote(
            x_next.at[block],
            x_next.at[block],
            xn_ss.at[(block // group) * group + off],
            xn_rs.at[block],
            place(lax.rem(member + off, group)),
        )

    slot = lax.rem(me, per_tensor)

    def state_copy(block):
        return remote(
            x_next.at[block],
            state_buf.at[slot],
            st_ss.at[block // group],
            st_rs.at[slot],
            {"section": layer, "dp": block, "tensor": me // per_tensor},
        )

    def state_local(block):
        return pltpu.make_async_copy(x_next.at[block], state_buf.at[slot], st_rs.at[slot])

    def finish(block):
        @pl.when(lax.rem(block, group) == member)
        def _():
            sum_now = part_send[block].astype(F32)
            for off in range(1, group):
                part_landing(block, off).wait_recv()
                sum_now = sum_now + part_recv[
                    block // group, lax.rem(member + off, group)
                ].astype(F32)
            x_next[block] = (x_ref[block].astype(F32) + sum_now).astype(BF16)
            if not is_last:
                for off in range(1, group):
                    next_copy(block, off).start()
            local = state_is_local(block)

            @pl.when(local)
            def _():
                state_local(block).start()

            @pl.when(jnp.logical_not(local))
            def _():
                state_copy(block).start()

    waiting = []

    def finish_oldest():
        valid, block = waiting.pop(0)
        if valid is None:
            finish(block)
        else:
            pl.when(valid)(lambda: finish(block))

    def use(block):
        store(block).start()
        part_send[block] = jnp.dot(
            hid[block], down_ref[...], preferred_element_type=F32
        ).astype(BF16)

        @pl.when(lax.rem(block, group) != member)
        def _():
            part_copy(block).start()

    def queue(valid, block):
        waiting.append((valid, block))
        if len(waiting) > 3:
            finish_oldest()

    last = outer - 1

    def start_hops(j):
        @pl.when((z - j >= 0) & (z < last))
        def _():
            hop(z - j, z + 1, up_ss, up_rs, j).start()

        @pl.when((z + j <= last) & (z > 0))
        def _():
            hop(z + j, z - 1, dn_ss, dn_rs, j).start()

    def use_peers(j):
        if j == 0:
            expect(z, 0).wait_recv()
            use(z * inner + peer)
            queue(None, z * inner + peer)
            return
        for valid, origin, sem_id in (
            (z - j >= 0, z - j, j),
            (z + j <= last, z + j, last + j),
        ):

            @pl.when(valid)
            def _():
                expect(origin, sem_id).wait_recv()
                use(origin * inner + peer)

            queue(valid, origin * inner + peer)

    start_hops(0)
    forward(z, 0).start()
    use(me)
    queue(None, me)
    for j in range(1, outer):
        above, below = z - j >= 0, z + j <= last

        @pl.when(above)
        def _():
            landing(z - j, up_ss, up_rs, j - 1).wait_recv()
            forward(z - j, j).start()

        @pl.when(below)
        def _():
            landing(z + j, dn_ss, dn_rs, j - 1).wait_recv()
            forward(z + j, last + j).start()

        if j < last:
            start_hops(j)
        for valid, origin in ((above, z - j), (below, z + j)):
            pl.when(valid)(lambda: use(origin * inner + x))
            queue(valid, origin * inner + x)
        use_peers(j - 1)
    use_peers(last)
    while waiting:
        finish_oldest()

    if not is_last:
        for block in range(dp_count):

            @pl.when(block % group != member)
            def _():
                next_copy(block, 0).wait_recv()

        pltpu.make_async_copy(x_next, x_out, end_sem.at[0]).start()

    @pl.when(core == layer)
    def _():
        stores = []
        for q in range(per_tensor):
            pltpu.make_async_copy(x_next.at[0], state_buf.at[q], st_rs.at[q]).wait()
            copy = pltpu.make_async_copy(
                state_buf.at[q],
                state_out.at[:, pl.ds(q * x_ref.shape[2], x_ref.shape[2])],
                end_sem.at[1 + q],
            )
            copy.start()
            stores.append(copy)
        for copy in stores:
            copy.wait()

    if not is_last:
        pltpu.make_async_copy(x_next, x_out, end_sem.at[0]).wait()
    for block in range(dp_count):

        @pl.when(block % group != member)
        def _():
            part_copy(block).wait_send()

    for i in range(owned):
        block = member + i * group
        if not is_last:
            for off in range(1, group):
                next_copy(block, off).wait_send()

        @pl.when(jnp.logical_not(state_is_local(block)))
        def _():
            state_copy(block).wait_send()

    for copy in list(x_copies.values()) + list(z_copies.values()) + sum_copies:
        copy.wait_send()
    forward(z, 0).wait_send()
    for j in range(last):

        @pl.when((z - j >= 0) & (z < last))
        def _():
            hop(z - j, z + 1, up_ss, up_rs, j).wait_send()

        @pl.when((z + j <= last) & (z > 0))
        def _():
            hop(z + j, z - 1, dn_ss, dn_rs, j).wait_send()

        @pl.when(z - 1 - j >= 0)
        def _():
            forward(z - 1 - j, 1 + j).wait_send()

        @pl.when(z + 1 + j <= last)
        def _():
            forward(z + 1 + j, outer + j).wait_send()

    for block in range(dp_count):
        store(block).wait()


def layer_step(layer, sizes, width, x, gain_row, up, down):
    sections, dp_count, tensors = sizes
    rows, slice_width = x.shape[1:]
    half = up.shape[1]
    inner = 2
    group = sections * tensors
    assert dp_count % inner == 0 and dp_count % group == 0
    outer = dp_count // inner
    per_tensor = dp_count // tensors
    is_last = layer == sections - 1
    dma = pltpu.SemaphoreType.DMA
    vmem = pl.BlockSpec(memory_space=pltpu.VMEM)
    hbm = pl.BlockSpec(memory_space=pl.ANY)
    wide = pltpu.VMEM((outer, rows, half), BF16)
    thin = pltpu.VMEM((dp_count, rows, slice_width), BF16)
    x_shape = x.shape if not is_last else (1, 8, 128)
    return pl.pallas_call(
        functools.partial(layer_kernel, sizes, inner, width, layer, is_last),
        name=f"layer{layer}",
        out_shape=(
            jax.ShapeDtypeStruct((dp_count, rows, half), BF16),
            jax.ShapeDtypeStruct(x_shape, BF16),
            jax.ShapeDtypeStruct((rows, per_tensor * slice_width), BF16),
        ),
        in_specs=[vmem] * 4,
        out_specs=(hbm, hbm, hbm),
        scratch_shapes=[
            thin,
            pltpu.VMEM((dp_count, 1, rows), F32),
            pltpu.VMEM((dp_count, 1, rows), F32),
            wide,
            wide,
            wide,
            wide,
            pltpu.VMEM((rows, half), F32),
            pltpu.VMEM((dp_count, rows, half), BF16),
            thin,
            pltpu.VMEM((dp_count // group, group, rows, slice_width), BF16),
            thin,
            pltpu.VMEM((per_tensor, rows, slice_width), BF16),
        ]
        + [dma((dp_count,))] * 2
        + [dma((outer,))] * 8
        + [dma((2 * outer,))] * 2
        + [dma((dp_count,))]
        + [dma((dp_count,))] * 4
        + [dma((dp_count // group,)), dma((per_tensor,)), dma((1 + per_tensor,))],
        compiler_params=pltpu.CompilerParams(collective_id=layer, has_side_effects=True),
    )(x, gain_row, up, down)


def front_kernel(
    sizes,
    tok_ref,
    gain_ref,
    up_ref,
    down_ref,
    cot_ref,
    x_out,
    gain_out0,
    gain_out1,
    up_out0,
    up_out1,
    down_out0,
    down_out1,
    cot_out,
    x_buf,
    gain_buf,
    up_buf,
    down_buf,
    cot_buf,
    tok_ss,
    tok_rs,
    ty_ss,
    tf_ss,
    tf_rs,
    cot_ss,
    cot_rs,
    cy_ss,
    cy_rs,
    gain_ss,
    gain_rs,
    w_ss,
    w_rs,
    own_sem,
    end_sem,
):
    sections, dp_count, tensors = sizes
    group = sections * tensors
    per_tensor = dp_count // tensors
    core = lax.axis_index("section")
    tensor = lax.axis_index("tensor")
    me = lax.axis_index("dp")
    other = 1 - core
    member = tensor * sections + core
    rows, slice_width = x_buf.shape[1:]
    half = up_buf.shape[2]
    half_rows = rows // sections
    part_rows = rows // tensors

    def place(index):
        return {"section": lax.rem(index, sections), "tensor": index // sections}

    barrier = pltpu.get_barrier_semaphore()

    def greet(target):
        pl.semaphore_signal(barrier, inc=1, device_id=target, device_id_type=MESH)

    for m in range(1, dp_count):
        greet({"dp": lax.rem(me + m, dp_count)})
    for off in range(1, group):
        greet(place(lax.rem(member + off, group)))
    feature_home = me // per_tensor
    at_home = feature_home == tensor
    pl.semaphore_wait(barrier, dp_count - 1 + group - 1)

    my_half = pl.ds(pl.multiple_of(core * half_rows, half_rows), half_rows)
    my_part = pl.ds(pl.multiple_of(tensor * part_rows, part_rows), part_rows)

    def columns(index, size):
        return pl.ds(pl.multiple_of(index * size, size), size)

    def token_copy(q):
        return remote(
            tok_ref.at[my_half, pl.ds(q * slice_width, slice_width)],
            x_buf.at[me, my_half],
            tok_ss.at[q],
            tok_rs.at[me],
            {"dp": tensor * per_tensor + q},
        )

    def token_local(q):
        return pltpu.make_async_copy(
            tok_ref.at[my_half, pl.ds(q * slice_width, slice_width)],
            x_buf.at[me, my_half],
            tok_rs.at[me],
        )

    def is_self(q):
        return tensor * per_tensor + q == me

    def token_share(source, off):
        return remote(
            x_buf.at[source, my_half],
            x_buf.at[source, my_half],
            ty_ss.at[source * tensors + off],
            tok_rs.at[source],
            {"tensor": lax.rem(tensor + off, tensors)},
        )

    for q in range(per_tensor):

        @pl.when(is_self(q))
        def _():
            token_local(q).start()

        @pl.when(jnp.logical_not(is_self(q)))
        def _():
            token_copy(q).start()

    def gain_copy(off):
        return remote(
            gain_ref.at[:, columns(lax.rem(me, per_tensor), slice_width)],
            gain_buf.at[core],
            gain_ss.at[off],
            gain_rs.at[core],
            place(lax.rem(member + off, group)),
        )

    gain_local = pltpu.make_async_copy(
        gain_ref.at[:, columns(lax.rem(me, per_tensor), slice_width)],
        gain_buf.at[core],
        gain_rs.at[core],
    )

    @pl.when(at_home)
    def _():
        gain_local.start()
        for off in range(1, group):
            gain_copy(off).start()

    def up_half(index):
        if up_ref.shape[0] == sections:
            return up_ref.at[index]
        return up_ref.at[0, :, columns(index, half)]

    give_up = remote(
        up_half(other),
        up_buf.at[core],
        w_ss.at[0],
        w_rs.at[0],
        {"section": other},
    )
    give_up.start()
    own_up = pltpu.make_async_copy(
        up_half(core), up_buf.at[core], own_sem.at[0]
    )
    own_up.start()

    cot_copies = []
    for m in range(1, dp_count):
        target = lax.rem(me + m, dp_count)
        copy = remote(
            cot_ref.at[0, my_part, columns(target, slice_width)],
            cot_buf.at[me, my_part],
            cot_ss.at[m],
            cot_rs.at[m],
            {"dp": target},
        )
        copy.start()
        cot_copies.append(copy)
    cot_local = pltpu.make_async_copy(
        cot_ref.at[0, my_part, columns(me, slice_width)], cot_buf.at[me, my_part], own_sem.at[2]
    )
    cot_local.start()

    give_down = remote(
        down_ref.at[0, columns(other, half), :],
        down_buf.at[core],
        w_ss.at[1],
        w_rs.at[1],
        {"section": other},
    )
    give_down.start()
    own_down = pltpu.make_async_copy(
        down_ref.at[0, columns(core, half), :], down_buf.at[core], own_sem.at[1]
    )
    own_down.start()

    def token_forward(source):
        return remote(
            x_buf.at[source, my_half],
            x_buf.at[source, my_half],
            tf_ss.at[source],
            tf_rs.at[source],
            {"section": other},
        )

    for source in range(dp_count):
        pltpu.make_async_copy(
            x_buf.at[source, my_half], x_buf.at[source, my_half], tok_rs.at[source]
        ).wait()

        @pl.when(at_home)
        def _():
            for off in range(1, tensors):
                token_share(source, off).start()

        token_forward(source).start()

    ends = []

    def put(src, dst):
        copy = pltpu.make_async_copy(src, dst, end_sem.at[len(ends)])
        copy.start()
        ends.append(copy)

    own_up.wait()
    give_up.wait_recv()
    put(up_buf.at[0], up_out0)
    put(up_buf.at[1], up_out1)
    own_down.wait()
    give_down.wait_recv()
    put(down_buf.at[0], down_out0)
    put(down_buf.at[1], down_out1)
    for layer in range(sections):
        pltpu.make_async_copy(
            gain_buf.at[layer], gain_buf.at[layer], gain_rs.at[layer]
        ).wait()
    put(gain_buf.at[0], gain_out0)
    put(gain_buf.at[1], gain_out1)

    def cot_share(m, off):
        source = lax.rem(me + dp_count - m, dp_count)
        return remote(
            cot_buf.at[source, my_part],
            cot_buf.at[source, my_part],
            cy_ss.at[m * tensors + off],
            cy_rs.at[m * tensors + off],
            {"tensor": lax.rem(tensor + off, tensors)},
        )

    for m in range(dp_count):
        if m == 0:
            cot_local.wait()
        else:
            cot_copies[m - 1].wait_recv()
        for off in range(1, tensors):
            cot_share(m, off).start()

    for source in range(dp_count):
        token_forward(source).wait_recv()
    put(x_buf, x_out)
    for m in range(dp_count):
        for off in range(1, tensors):
            cot_share(m, off).wait_recv()
    put(cot_buf, cot_out)

    for q in range(per_tensor):

        @pl.when(jnp.logical_not(is_self(q)))
        def _():
            token_copy(q).wait_send()

    @pl.when(at_home)
    def _():
        for off in range(1, group):
            gain_copy(off).wait_send()
        for source in range(dp_count):
            for off in range(1, tensors):
                token_share(source, off).wait_send()

    give_up.wait_send()
    give_down.wait_send()
    for copy in cot_copies:
        copy.wait_send()
    for source in range(dp_count):
        token_forward(source).wait_send()
    for m in range(dp_count):
        for off in range(1, tensors):
            cot_share(m, off).wait_send()
    for copy in ends:
        copy.wait()


def front(sizes, tokens, gain, w_up, w_down, cotangent):
    sections, dp_count, tensors = sizes
    assert sections == 2
    group = sections * tensors
    per_tensor = dp_count // tensors
    rows, own_width = tokens.shape
    slice_width = own_width // per_tensor
    depth = w_up.shape[1]
    half = w_up.shape[2] // sections
    dma = pltpu.SemaphoreType.DMA
    hbm = pl.BlockSpec(memory_space=pl.ANY)
    if half % 128:
        w_up = w_up[0].reshape(depth, sections, half).transpose(1, 0, 2)

    def shape(*dims, dtype=BF16):
        return jax.ShapeDtypeStruct(dims, dtype)

    return pl.pallas_call(
        functools.partial(front_kernel, sizes),
        name="front",
        out_shape=(
            shape(dp_count, rows, slice_width),
            shape(1, slice_width, dtype=F32),
            shape(1, slice_width, dtype=F32),
            shape(depth, half),
            shape(depth, half),
            shape(half, slice_width),
            shape(half, slice_width),
            shape(dp_count, rows, slice_width),
        ),
        in_specs=[hbm] * 5,
        out_specs=(hbm,) * 8,
        scratch_shapes=[
            pltpu.VMEM((dp_count, rows, slice_width), BF16),
            pltpu.VMEM((sections, 1, slice_width), F32),
            pltpu.VMEM((sections, depth, half), BF16),
            pltpu.VMEM((sections, half, slice_width), BF16),
            pltpu.VMEM((dp_count, rows, slice_width), BF16),
            dma((dp_count,)),
            dma((dp_count,)),
            dma((dp_count * tensors,)),
            dma((dp_count,)),
            dma((dp_count,)),
            dma((dp_count,)),
            dma((dp_count,)),
            dma((dp_count * tensors,)),
            dma((dp_count * tensors,)),
            dma((group,)),
            dma((sections,)),
            dma((2,)),
            dma((2,)),
            dma((3,)),
            dma((8,)),
        ],
        compiler_params=pltpu.CompilerParams(collective_id=sections, has_side_effects=True),
    )(tokens, gain.astype(F32), w_up, w_down, cotangent)


def body(tokens, gain, w_up, w_down, cotangent):
    core = lax.axis_index("section")
    layers = lax.axis_size("section")
    dp_count = lax.axis_size("dp")
    tensor_count = lax.axis_size("tensor")
    rows, own_width = tokens.shape
    width = own_width * tensor_count
    half = w_up.shape[2] // layers
    all_rows = rows * dp_count
    sizes = (layers, dp_count, tensor_count)

    def swap(array):
        return lax.ppermute(array, "section", [(0, 1), (1, 0)])

    def both(own, got):
        return (jnp.where(core == 0, own, got), jnp.where(core == 0, got, own))

    x, *rest = front(sizes, tokens, gain, w_up, w_down, cotangent)
    gains, up_parts, down_parts = rest[0:2], rest[2:4], rest[4:6]
    cot_mine = rest[6].reshape(all_rows, -1)

    states = []
    hiddens = []
    for layer in range(layers):
        hidden, x, state = layer_step(
            layer, sizes, width, x, gains[layer], up_parts[layer], down_parts[layer]
        )
        hiddens.append(hidden.reshape(all_rows, half))
        states.append(state)
    state = jnp.where(core == 0, states[0], states[1])

    hid_keep = jnp.where(core == 0, hiddens[0], hiddens[1])
    hid_got = swap(jnp.where(core == 0, hiddens[1], hiddens[0]))
    hid_parts = both(hid_keep, hid_got)
    hidden_whole = jnp.concatenate(hid_parts, axis=1)
    grad = lax.dot_general(
        hidden_whole, cot_mine, (((0,), (0,)), ((), ())), preferred_element_type=F32
    ).astype(BF16)
    return (state[None], grad[None])


def solution(mesh):
    placed = (
        P("dp", "tensor"),
        P("section", "tensor"),
        P("section", "dp", "tensor"),
        P("section", "tensor", "dp"),
        P("section", "dp", None),
    )
    return jax.shard_map(
        body,
        mesh=mesh,
        in_specs=placed,
        out_specs=(P("section", "dp", "tensor"), P("section", "tensor", "dp")),
        check_vma=False,
    )
```
